32 devices in a mesh: dp: 4 (over z), mp: 8 (over y, x, core).
Axes of the slice: x: 2, y: 2, z: 4, core: 2. Of those that a mesh axis runs over, the one named last changes fastest.
Arguments:
- tokens: bfloat16 [4096, 4096], P('dp', 'mp'), may hold values from -6 to 6
- decay: float32 [4096, 16], P('dp'), may hold values from 0.75 to 1, as said below
- state: float32 [128, 256, 8192], P('dp', None, 'mp'), may hold values from -24 to 24
- w_query: bfloat16 [4096, 4096], P(None, 'mp'), may hold values from -0.09375 to 0.09375
- w_key: bfloat16 [4096, 4096], P(None, 'mp'), may hold values from -0.09375 to 0.09375
- w_value: bfloat16 [4096, 8192], P(None, 'mp'), may hold values from -0.09375 to 0.09375
- w_gate: bfloat16 [4096, 8192], P(None, 'mp'), may hold values from -0.09375 to 0.09375
- w_out: bfloat16 [8192, 4096], P('mp'), may hold values from -0.09375 to 0.09375
- norm_gain: float32 [8192], P('mp'), may hold values from 0.25 to 1.75
Outputs:
- layer_out: bfloat16 [4096, 4096], P('dp', 'mp')
- new_state: float32 [128, 256, 8192], P('dp', None, 'mp')
The draws below stay inside these ranges and needn't reach their ends.
Inputs may be any that keep to these rules, and one draw needn't show every extreme that they name: `decay`: each head has its own base rate over all tokens, varied somewhat from token to token.
All inputs are finite; a program needn't handle non-finite values.
Results may differ from the reference program's by a relative error of at most 0.0071.
Values may be sent and summed in bfloat16 or wider, within the bound.
A program may use at most 256 MiB of HBM per device.

```python
import jax
import jax.numpy as jnp
from jax import lax

D = 4096
H = 16
HEAD = 256
VHEAD = 512
NEW = 32
BATCH = 128
TOKENS = 4096


def draw_decay(key, part):
    base_key, jitter_key = jax.random.split(key)
    base_low = 0.85
    jitter_low = 0.93
    base_rate = jnp.exp(jax.random.uniform(base_key, (H,), jnp.float32, jnp.log(base_low), jnp.log(0.999)))
    jitter = jax.random.uniform(jitter_key, (TOKENS, H), jnp.float32, jitter_low, 1.0)
    return base_rate[None, :] * jitter


def with_spikes(result, key, source, target, parts, factor):
    owner, partner = [(jnp.arange(result.shape[position]) // (result.shape[position] // parts)).reshape([-1 if axis == position else 1 for axis in range(result.ndim)]) for position in (source, target)]
    chosen = jax.random.permutation(key, parts)[partner]
    strong = (owner == chosen) | (owner == (partner + parts // 2) % parts)
    return jnp.where(strong, factor * result, result)


def block_levels(rng, dims, shards, low, largest):
    level = 1.0
    for position, shards_of in shards:
        heights = jax.random.uniform(jax.random.fold_in(jax.random.fold_in(rng, 6), position), (shards_of,), jnp.float32, low / len(shards), largest / len(shards))
        level = level * jnp.repeat(jnp.exp(heights), dims[position] // shards_of).reshape((-1,) + (1,) * (len(dims) - 1 - position))
    return level


def gaussian(rng, shape, scale, most, cuts=(), held_as=jnp.bfloat16):
    values = scale * jax.random.normal(rng, shape, jnp.float32)
    if cuts:
        values = values * block_levels(rng, shape, cuts, -0.22, 0.18)
    return jnp.clip(values, -most, most).astype(held_as)


def bell_draw_with(own_key, shape, width, most, pieces, heavy, held_as=jnp.bfloat16):
    result = width * jax.random.normal(own_key, shape, jnp.float32)
    if pieces:
        result = result * block_levels(own_key, shape, pieces, -0.22, 0.18)
    return jnp.clip(with_spikes(result, jax.random.fold_in(own_key, 3), *heavy), -most, most).astype(held_as)


def setup_inputs(seed: int = 0) -> dict:
    arg_keys = jax.random.split(jax.random.key(seed), 10)
    return {
        "tokens": gaussian(arg_keys[0], (TOKENS, D), 1.0, 6.0, ((0, 4), (1, 8))),
        "decay": draw_decay(jax.random.fold_in(arg_keys[9], 71), 0),
        "state": gaussian(arg_keys[2], (BATCH, HEAD, H * VHEAD), 4.0, 24.0, ((0, 4), (2, 8)), jnp.float32),
        "w_query": gaussian(arg_keys[3], (D, H * HEAD), D ** -0.5, 0.09375, ((1, 8),)),
        "w_key": gaussian(arg_keys[4], (D, H * HEAD), D ** -0.5, 0.09375, ((1, 8),)),
        "w_value": gaussian(arg_keys[5], (D, H * VHEAD), D ** -0.5, 0.09375, ((1, 8),)),
        "w_gate": gaussian(arg_keys[6], (D, H * VHEAD), D ** -0.5, 0.09375, ((1, 8),)),
        "w_out": bell_draw_with(arg_keys[7], (H * VHEAD, D), (H * VHEAD) ** -0.5, 0.09375, ((0, 8),), (0, 1, 8, 2.0)),
        "norm_gain": jnp.clip(1.0 + 0.15 * jax.random.normal(arg_keys[8], (H * VHEAD,), jnp.float32), 0.25, 1.75),
    }


EPS = 0.1

def one_sequence(packed):
    query, key_proj, value_proj, decay_rates, old_state = packed
    highest = lax.Precision.HIGHEST
    log_cumul = jnp.cumsum(jnp.log(decay_rates), axis=0)
    from_state = jnp.einsum('nhk,khv->nhv', query.astype(jnp.float32), old_state, precision=highest)
    scores = jnp.einsum('nhk,mhk->hnm', query.astype(jnp.float32), key_proj.astype(jnp.float32), precision=highest)
    along = log_cumul.T
    log_gap = along[:, :, None] - along[:, None, :]
    causal = jnp.arange(NEW)[:, None] >= jnp.arange(NEW)[None, :]
    factor = jnp.where(causal, jnp.exp(jnp.where(causal, log_gap, 0.0)), 0.0)
    weights = (scores * factor).astype(jnp.bfloat16)
    in_block = jnp.einsum('hnm,mhv->nhv', weights.astype(jnp.float32), value_proj.astype(jnp.float32), precision=highest)
    retained = jnp.exp(log_cumul)[:, :, None] * from_state + in_block
    final_log = log_cumul[-1]
    carry_scale = jnp.exp(final_log[None, :] - log_cumul)
    decayed_keys = key_proj.astype(jnp.float32) * carry_scale[:, :, None]
    fresh = jnp.einsum('nhk,nhv->khv', decayed_keys, value_proj.astype(jnp.float32), precision=highest)
    new_state = jnp.exp(final_log)[None, :, None] * old_state + fresh
    return (retained, new_state)

def reference(tokens, decay, state, w_query, w_key, w_value, w_gate, w_out, norm_gain):
    query = (jnp.dot(tokens, w_query, preferred_element_type=jnp.float32) * HEAD ** (-0.5)).astype(jnp.bfloat16)
    key_proj = jnp.dot(tokens, w_key, preferred_element_type=jnp.float32).astype(jnp.bfloat16)
    value_proj = jnp.dot(tokens, w_value, preferred_element_type=jnp.float32).astype(jnp.bfloat16)
    gate_proj = jnp.dot(tokens, w_gate, preferred_element_type=jnp.float32)
    packed = (query.reshape(BATCH, NEW, H, HEAD), key_proj.reshape(BATCH, NEW, H, HEAD), value_proj.reshape(BATCH, NEW, H, VHEAD), decay.reshape(BATCH, NEW, H), state.reshape(BATCH, HEAD, H, VHEAD))
    retained, new_state = lax.map(one_sequence, packed)
    retained = retained.reshape(TOKENS, H, VHEAD)
    centre = lax.optimization_barrier(jnp.mean(retained, axis=-1))
    deviation = retained - centre[..., None]
    variance = lax.optimization_barrier(jnp.mean(deviation * deviation, axis=-1))
    normed = deviation * lax.rsqrt(variance + EPS)[..., None]
    gated_out = (normed.reshape(TOKENS, H * VHEAD) * norm_gain * jax.nn.silu(gate_proj)).astype(jnp.bfloat16)
    layer_out = jnp.dot(gated_out, w_out, preferred_element_type=jnp.float32).astype(jnp.bfloat16)
    return (layer_out, new_state.reshape(BATCH, HEAD, H * VHEAD))
```

```python
import functools

import jax
import jax.numpy as jnp
from jax import lax
from jax.experimental import pallas as pl
from jax.experimental.pallas import tpu as pltpu
from jax.sharding import PartitionSpec as P

HEAD = 256
VHEAD = 512
NEW = 32


EPS = 0.1


def partner(shard, axis, bit):
    return lax.ppermute(shard, axis, [(i, i ^ 1 << bit) for i in range(lax.axis_size(axis))])


def split_heads(tokens, decay, state, w_query, w_key, w_value, w_gate, w_out, norm_gain):
    highest = lax.Precision.HIGHEST
    tok_rows = tokens.shape[0]
    qk_columns = w_query.shape[1]
    v_columns = w_value.shape[1]
    head_span = max(1, HEAD // qk_columns)
    groups = max(1, qk_columns // HEAD)
    qk_width = qk_columns // groups
    v_width = v_columns // groups
    sequences = tok_rows // NEW
    bit_count = head_span.bit_length() - 1
    device_index = lax.axis_index("mp")
    first_head = device_index * qk_columns // HEAD
    qk_zeros = jnp.zeros((tok_rows, qk_columns), jnp.float32)
    v_zeros = jnp.zeros((tok_rows, v_columns), jnp.float32)
    carried = (qk_zeros, qk_zeros, v_zeros, v_zeros)
    segment = lax.all_gather(tokens, "mp", axis=1, tiled=True)
    updated = []
    for running, weight in zip(carried, (w_query, w_key, w_value, w_gate)):
        updated.append(jnp.dot(segment, weight, preferred_element_type=jnp.float32))
    query, key_proj, value_proj, gate_proj = tuple(updated)
    query = (query * HEAD ** (-0.5)).astype(jnp.bfloat16).reshape(tok_rows, groups, qk_width)
    key_proj = key_proj.astype(jnp.bfloat16).reshape(tok_rows, groups, qk_width)
    value_proj = value_proj.astype(jnp.bfloat16)
    for bit_number in range(bit_count):
        other_query, other_key = partner((query, key_proj), "mp", bit_number)
        upper_half = device_index >> bit_number & 1 == 1
        query = jnp.where(
            upper_half,
            jnp.concatenate([other_query, query], 2),
            jnp.concatenate([query, other_query], 2),
        )
        key_proj = jnp.where(
            upper_half,
            jnp.concatenate([other_key, key_proj], 2),
            jnp.concatenate([key_proj, other_key], 2),
        )
    query_block = query.reshape(sequences, NEW, groups, HEAD)
    key_block = key_proj.reshape(sequences, NEW, groups, HEAD)
    value_block = value_proj.reshape(sequences, NEW, groups, v_width)
    decay_rates = lax.dynamic_slice_in_dim(decay, first_head, groups, 1).reshape(
        sequences, NEW, groups
    )
    log_cumul = jnp.cumsum(jnp.log(decay_rates), axis=1)
    old_state = state.reshape(sequences, HEAD, groups, v_width)
    from_state = jnp.einsum(
        "bngk,bkgv->bngv", query_block.astype(jnp.float32), old_state, precision=highest
    )
    scores = jnp.einsum(
        "bngk,bmgk->bgnm", query_block, key_block, preferred_element_type=jnp.float32
    )
    along = jnp.transpose(log_cumul, (0, 2, 1))
    log_gap = along[:, :, :, None] - along[:, :, None, :]
    causal = jnp.arange(NEW)[:, None] >= jnp.arange(NEW)[None, :]
    factor = jnp.where(causal, jnp.exp(jnp.where(causal, log_gap, 0.0)), 0.0)
    weights = (scores * factor).astype(jnp.bfloat16)
    in_block = jnp.einsum(
        "bgnm,bmgv->bngv", weights, value_block, preferred_element_type=jnp.float32
    )
    retained = jnp.exp(log_cumul)[..., None] * from_state + in_block
    final_log = log_cumul[:, -1, :]
    carry_scale = jnp.exp(final_log[:, None, :] - log_cumul)
    decayed_keys = key_block.astype(jnp.float32) * carry_scale[..., None]
    fresh = jnp.einsum(
        "bngk,bngv->bkgv", decayed_keys, value_block.astype(jnp.float32), precision=highest
    )
    new_state = jnp.exp(final_log)[:, None, :, None] * old_state + fresh
    new_state = new_state.reshape(sequences, HEAD, v_columns)
    retained = retained.reshape(tok_rows, groups, v_width)
    running = jnp.sum(retained, axis=-1)
    squares = jnp.sum(retained * retained, axis=-1)
    for bit_number in range(bit_count):
        other_sum, other_square = partner((running, squares), "mp", bit_number)
        running = running + other_sum
        squares = squares + other_square
    centre = running / VHEAD
    variance = squares / VHEAD - centre * centre
    deviation = retained - centre[..., None]
    normed = deviation * lax.rsqrt(variance + EPS)[..., None]
    gated_out = (normed.reshape(tok_rows, v_columns) * norm_gain * jax.nn.silu(gate_proj)).astype(
        jnp.bfloat16
    )
    partial_terms = jnp.dot(gated_out, w_out, preferred_element_type=jnp.float32)
    layer_out = lax.psum_scatter(partial_terms, "mp", scatter_dimension=1, tiled=True).astype(
        jnp.bfloat16
    )
    return (layer_out, new_state)


CHUNKS = 4
PER_STEP = 2
TILE = 512


def retention_step(
    per_step, groups, c_col, c_row, q, k, v, gate, gain, state, *rest
):
    gated, new_state = rest[-2:]
    vw = v.shape[1] // groups
    rows = lax.broadcasted_iota(jnp.int32, (NEW, NEW), 0)
    cols = lax.broadcasted_iota(jnp.int32, (NEW, NEW), 1)
    causal = rows >= cols
    for s in range(per_step):
        at = slice(s * NEW, (s + 1) * NEW)
        for g in range(groups):
            vs = slice(g * vw, (g + 1) * vw)
            ks = slice(g * HEAD, (g + 1) * HEAD)
            col = c_col[at, g : g + 1]
            row = c_row[s, g : g + 1, :]
            last = col[NEW - 1 : NEW, :]
            factor = jnp.where(causal, jnp.exp(jnp.where(causal, col - row, 0.0)), 0.0)
            query, key, value = q[at, ks], k[at, ks], v[at, vs]
            scores = lax.dot_general(
                query, key, (((1,), (1,)), ((), ())), preferred_element_type=jnp.float32
            )
            weights = (scores * factor).astype(jnp.bfloat16)
            old = state[s, :, vs]
            from_state = jnp.dot(
                query, old.astype(jnp.bfloat16), preferred_element_type=jnp.float32
            )
            in_block = jnp.dot(weights, value, preferred_element_type=jnp.float32)
            retained = jnp.exp(col) * from_state + in_block
            scaled = (key.astype(jnp.float32) * jnp.exp(last - col)).astype(jnp.bfloat16)
            fresh = lax.dot_general(
                scaled, value, (((0,), (0,)), ((), ())), preferred_element_type=jnp.float32
            )
            new_state[s, :, vs] = jnp.exp(last) * old + fresh
            centre = jnp.mean(retained, axis=1, keepdims=True)
            deviation = retained - centre
            variance = jnp.mean(deviation * deviation, axis=1, keepdims=True)
            normed = deviation * lax.rsqrt(variance + EPS)
            gates = gate[at, vs]
            silu = gates / (1.0 + jnp.exp(-gates))
            gated[at, vs] = (normed * gain[:, vs] * silu).astype(jnp.bfloat16)


def retention(chunk, chunks, c_col, c_row, q, k, v, gate, gain, state, previous):
    rows, groups = c_col.shape
    sequences = rows // NEW
    per_step = PER_STEP if sequences % PER_STEP == 0 else 1
    steps = sequences // per_step
    step_rows = per_step * NEW
    qk, vc = q.shape[1], v.shape[1]
    first = chunk * steps
    by_row = lambda width: pl.BlockSpec((step_rows, width), lambda i: (i, 0))
    state_spec = pl.BlockSpec((per_step, HEAD, vc), lambda i: (first + i, 0, 0))
    in_specs = [
        by_row(groups),
        pl.BlockSpec((per_step, groups, NEW), lambda i: (i, 0, 0)),
        by_row(qk),
        by_row(qk),
        by_row(vc),
        by_row(vc),
        pl.BlockSpec((1, vc), lambda i: (0, 0)),
        state_spec,
    ]
    operands = [c_col, c_row, q, k, v, gate, gain, state]
    aliases = {}
    if previous is not None:
        in_specs.append(pl.BlockSpec(memory_space=pl.ANY))
        aliases = {len(operands): 1}
        operands.append(previous)
    return pl.pallas_call(
        functools.partial(retention_step, per_step, groups),
        grid=(steps,),
        in_specs=in_specs,
        out_specs=[by_row(vc), state_spec],
        out_shape=[
            jax.ShapeDtypeStruct((rows, vc), jnp.bfloat16),
            jax.ShapeDtypeStruct(state.shape, jnp.float32),
        ],
        input_output_aliases=aliases,
        compiler_params=pltpu.CompilerParams(
            dimension_semantics=("arbitrary",), vmem_limit_bytes=40 << 20
        ),
        cost_estimate=pl.CostEstimate(
            flops=12 * rows * HEAD * vc,
            bytes_accessed=8 * sequences * HEAD * vc,
            transcendentals=rows * vc,
        ),
    )(*operands)


def partners(device):
    core = device % 2
    across_x = device + 2 - 4 * ((device // 2) % 2)
    across_y = device + 4 - 8 * (device // 4)
    near = across_x + core * (across_y - across_x)
    far = across_y + core * (across_x - across_y)
    return near, far, across_x + across_y - device, device + 1 - 2 * core


def meet(devices):
    barrier = pltpu.get_barrier_semaphore()
    for device in devices:
        pl.semaphore_signal(
            barrier, inc=1, device_id={"mp": device}, device_id_type=pl.DeviceIdType.MESH
        )
    pl.semaphore_wait(barrier, len(devices))


def remote(source, target, send, recv, device):
    return pltpu.make_async_remote_copy(
        src_ref=source,
        dst_ref=target,
        send_sem=send,
        recv_sem=recv,
        device_id={"mp": device},
        device_id_type=pl.DeviceIdType.MESH,
    )


def project_kernel(
    chunks,
    tokens,
    w_query,
    w_key,
    w_value,
    w_gate,
    query,
    key_proj,
    value_proj,
    gate_proj,
    gathered,
    wq,
    wk,
    wv,
    wg,
    q_held,
    k_held,
    v_held,
    g_held,
    load_sem,
    out_sem,
    send,
    recv,
):
    me = lax.axis_index("mp")
    near, far, diagonal, sibling = partners(me)
    sib_near, sib_far, sib_diagonal, _ = partners(sibling)
    rows, width = tokens.shape
    size = rows // chunks

    def block(device, r):
        return gathered.at[
            pl.ds(pl.multiple_of(r * size, size), size),
            pl.ds(pl.multiple_of(device * width, width), width),
        ]

    def copy(lane, source, target, r):
        there = block(source, r)
        return remote(there, there, send.at[lane, r], recv.at[lane, r], target)

    own = pltpu.make_async_copy(
        tokens, gathered.at[:, pl.ds(pl.multiple_of(me * width, width), width)], load_sem.at[0]
    )
    own.start()
    loads = [
        pltpu.make_async_copy(source, held, load_sem.at[1 + n])
        for n, (source, held) in enumerate(
            ((w_query, wq), (w_key, wk), (w_value, wv), (w_gate, wg))
        )
    ]
    for load in loads:
        load.start()
    meet((near, far, sibling))
    own.wait()
    for r in range(chunks):
        copy(0, me, near, r).start()
        if r == 0:
            copy(1, me, far, r).start()
        copy(3, me, sibling, r).start()

    def forward(r):
        copy(0, near, near, r).wait_recv()
        copy(2, near, far, r).start()
        copy(4, near, sibling, r).start()

        @pl.when(r + 1 < chunks)
        def _():
            copy(1, me, far, r + 1).start()

    def project(r, held, weight, scale, out, n):
        at = pl.ds(pl.multiple_of(r * size, size), size)
        for col in range(0, weight.shape[1], TILE):
            cols = slice(col, min(col + TILE, weight.shape[1]))
            part = jnp.dot(gathered[at, :], weight[:, cols], preferred_element_type=jnp.float32)
            if scale is not None:
                part = part * scale
            held[at, cols] = part.astype(held.dtype)
        pltpu.make_async_copy(held.at[at, :], out.at[at, :], out_sem.at[n, r]).start()

    sets = (
        (q_held, wq, HEAD ** (-0.5), query),
        (k_held, wk, None, key_proj),
        (v_held, wv, None, value_proj),
        (g_held, wg, None, gate_proj),
    )
    forward(0)

    def step(r, carry):
        copy(1, far, far, r).wait_recv()
        copy(5, far, sibling, r).start()
        copy(2, diagonal, far, r).wait_recv()
        copy(6, diagonal, sibling, r).start()

        @pl.when(r + 1 < chunks)
        def _():
            forward(r + 1)

        copy(3, sibling, sibling, r).wait_recv()
        copy(4, sib_near, sibling, r).wait_recv()
        copy(5, sib_far, sibling, r).wait_recv()
        copy(6, sib_diagonal, sibling, r).wait_recv()
        for n, (held, weight, scale, out) in enumerate(sets):

            @pl.when(r == 0)
            def _():
                loads[n].wait()

            project(r, held, weight, scale, out, n)
        return carry

    lax.fori_loop(0, chunks, step, 0)

    def drain(r, carry):
        at = pl.ds(pl.multiple_of(r * size, size), size)
        for lane, (source, target) in enumerate(
            (
                (me, near),
                (me, far),
                (near, far),
                (me, sibling),
                (near, sibling),
                (far, sibling),
                (diagonal, sibling),
            )
        ):
            copy(lane, source, target, r).wait_send()
        for n, (held, weight, scale, out) in enumerate(sets):
            pltpu.make_async_copy(held.at[at, :], out.at[at, :], out_sem.at[n, r]).wait()
        return carry

    lax.fori_loop(0, chunks, drain, 0)


def gather_project(tokens, w_query, w_key, w_value, w_gate):
    rows, width = tokens.shape
    depth, qk = w_query.shape
    vc = w_value.shape[1]
    chunks = CHUNKS
    shapes = [
        ((rows, qk), jnp.bfloat16),
        ((rows, qk), jnp.bfloat16),
        ((rows, vc), jnp.bfloat16),
        ((rows, vc), jnp.float32),
    ]
    anywhere = pl.BlockSpec(memory_space=pl.ANY)
    return pl.pallas_call(
        functools.partial(project_kernel, chunks),
        in_specs=[anywhere] * 5,
        out_specs=[anywhere] * 4,
        out_shape=[jax.ShapeDtypeStruct(*shape) for shape in shapes],
        scratch_shapes=[
            pltpu.VMEM((rows, depth), jnp.bfloat16),
            pltpu.VMEM((depth, qk), jnp.bfloat16),
            pltpu.VMEM((depth, qk), jnp.bfloat16),
            pltpu.VMEM((depth, vc), jnp.bfloat16),
            pltpu.VMEM((depth, vc), jnp.bfloat16),
        ]
        + [pltpu.VMEM(*shape) for shape in shapes]
        + [
            pltpu.SemaphoreType.DMA((5,)),
            pltpu.SemaphoreType.DMA((4, chunks)),
            pltpu.SemaphoreType.DMA((7, chunks)),
            pltpu.SemaphoreType.DMA((7, chunks)),
        ],
        compiler_params=pltpu.CompilerParams(
            collective_id=0, has_side_effects=True, vmem_limit_bytes=56 << 20
        ),
    )(tokens, w_query, w_key, w_value, w_gate)


def output_kernel(
    chunks,
    gated,
    w_out,
    layer_out,
    gated_held,
    w_held,
    to_sibling,
    from_sibling,
    outgoing,
    incoming,
    total,
    load_sem,
    send,
    recv,
):
    me = lax.axis_index("mp")
    near, far, diagonal, sibling = partners(me)
    sib_near, sib_far, sib_diagonal, _ = partners(sibling)
    width = layer_out.shape[1]
    rows = gated.shape[0]
    size = rows // chunks
    loads = [
        pltpu.make_async_copy(gated, gated_held, load_sem.at[0]),
        pltpu.make_async_copy(w_out, w_held, load_sem.at[1]),
    ]
    for load in loads:
        load.start()
    meet((near, far, sibling))
    for load in loads:
        load.wait()
    mine = (me, near, far, diagonal)
    theirs = (sibling, sib_near, sib_far, sib_diagonal)

    def at(r):
        return pl.ds(pl.multiple_of(r * size, size), size)

    def share(dest, r):
        return jnp.dot(
            gated_held[at(r), :],
            w_held[:, pl.ds(pl.multiple_of(dest * width, width), width)],
            preferred_element_type=jnp.float32,
        )

    def swap(j, r):
        return remote(
            to_sibling.at[j, at(r), :],
            from_sibling.at[j, at(r), :],
            send.at[j, r],
            recv.at[j, r],
            sibling,
        )

    def hop(lane, r):
        return remote(
            outgoing.at[lane, at(r), :],
            incoming.at[lane, at(r), :],
            send.at[4 + lane, r],
            recv.at[4 + lane, r],
            near if lane == 0 else far,
        )

    for j in (3, 2, 1, 0):

        def give(r, carry):
            to_sibling[j, at(r), :] = share(theirs[j], r).astype(jnp.bfloat16)
            swap(j, r).start()
            return carry

        def combine(r, carry):
            part = share(mine[j], r)
            swap(j, r).wait_recv()
            part = part + from_sibling[j, at(r), :].astype(jnp.float32)
            if j == 1:
                hop(2, r).wait_recv()
                part = part + incoming[2, at(r), :].astype(jnp.float32)
            if j == 0:
                total[at(r), :] = part
            else:
                outgoing[j - 1, at(r), :] = part.astype(jnp.bfloat16)
                hop(j - 1, r).start()
            return carry

        lax.fori_loop(0, chunks, give, 0)
        lax.fori_loop(0, chunks, combine, 0)

    def finish(r, carry):
        hop(1, r).wait_recv()
        hop(0, r).wait_recv()
        layer_out[at(r), :] = (
            total[at(r), :]
            + incoming[0, at(r), :].astype(jnp.float32)
            + incoming[1, at(r), :].astype(jnp.float32)
        ).astype(jnp.bfloat16)
        for j in range(4):
            swap(j, r).wait_send()
        for lane in range(3):
            hop(lane, r).wait_send()
        return carry

    lax.fori_loop(0, chunks, finish, 0)


def project_out(gated, w_out, width):
    rows = gated.shape[0]
    chunks = CHUNKS
    anywhere = pl.BlockSpec(memory_space=pl.ANY)
    return pl.pallas_call(
        functools.partial(output_kernel, chunks),
        in_specs=[anywhere] * 2,
        out_specs=pl.BlockSpec(memory_space=pltpu.VMEM),
        out_shape=jax.ShapeDtypeStruct((rows, width), jnp.bfloat16),
        scratch_shapes=[
            pltpu.VMEM(gated.shape, jnp.bfloat16),
            pltpu.VMEM(w_out.shape, jnp.bfloat16),
            pltpu.VMEM((4, rows, width), jnp.bfloat16),
            pltpu.VMEM((4, rows, width), jnp.bfloat16),
            pltpu.VMEM((3, rows, width), jnp.bfloat16),
            pltpu.VMEM((3, rows, width), jnp.bfloat16),
            pltpu.VMEM((rows, width), jnp.float32),
            pltpu.SemaphoreType.DMA((2,)),
            pltpu.SemaphoreType.DMA((7, chunks)),
            pltpu.SemaphoreType.DMA((7, chunks)),
        ],
        compiler_params=pltpu.CompilerParams(
            collective_id=1, has_side_effects=True, vmem_limit_bytes=56 << 20
        ),
    )(gated, w_out)


def whole_heads(tokens, decay, state, w_query, w_key, w_value, w_gate, w_out, norm_gain):
    tok_rows = tokens.shape[0]
    groups = w_query.shape[1] // HEAD
    sequences = tok_rows // NEW
    first_head = lax.axis_index("mp") * groups
    logs = jnp.log(lax.dynamic_slice_in_dim(decay, first_head, groups, 1))
    logs = logs.reshape(sequences, NEW, groups)
    causal = jnp.arange(NEW)[:, None] >= jnp.arange(NEW)[None, :]
    cumul = jnp.sum(jnp.where(causal[None, :, :, None], logs[:, None], 0.0), axis=2)
    c_col = cumul.reshape(tok_rows, groups)
    c_row = jnp.transpose(cumul, (0, 2, 1))
    query, key_proj, value_proj, gate_proj = gather_project(
        tokens, w_query, w_key, w_value, w_gate
    )
    gated_out, new_state = retention(
        0,
        1,
        c_col,
        c_row,
        query,
        key_proj,
        value_proj,
        gate_proj,
        norm_gain.reshape(1, -1),
        state,
        None,
    )
    return (project_out(gated_out, w_out, tokens.shape[1]), new_state)


def per_device(tokens, decay, state, w_query, *rest):
    whole = w_query.shape[1] % HEAD == 0 and lax.axis_size("mp") == 8
    path = whole_heads if whole else split_heads
    return path(tokens, decay, state, w_query, *rest)


def solution(mesh):
    placed = (
        P("dp", "mp"),
        P("dp", None),
        P("dp", None, "mp"),
        P(None, "mp"),
        P(None, "mp"),
        P(None, "mp"),
        P(None, "mp"),
        P("mp", None),
        P("mp"),
    )
    return jax.shard_map(
        per_device,
        mesh=mesh,
        in_specs=placed,
        out_specs=(P("dp", "mp"), P("dp", None, "mp")),
        check_vma=False,
    )
```
